8 devices in a mesh: dp: 2 (over z, y), pp: 4 (over x, core).
Axes of the slice: x: 2, y: 2, z: 1, core: 2. Of those that a mesh axis runs over, the one named last changes fastest.
Arguments:
- inputs: bfloat16 [512, 32, 1000], P('dp'), parts along dimension 0
- targets: bfloat16 [512, 32, 1000], P('dp'), parts along dimension 0
- w_in: bfloat16 [4, 4, 1000, 4000], P('dp', 'pp'), parts along dimension 0
- w_hid: bfloat16 [4, 4, 1000, 4000], P('dp', 'pp'), parts along dimension 0
- bias: float32 [4, 4, 4000], P('dp', 'pp'), parts along dimension 0
- h_init: float32 [4, 4, 256, 1000], P('dp', 'pp'), parts along dimension 0
- c_init: float32 [4, 4, 256, 1000], P('dp', 'pp'), parts along dimension 0
Outputs:
- output 1: float32 [2], P('dp'), parts along dimension 0
- output 2: float32 [4, 4, 1000, 4000], P('dp', 'pp'), parts along dimension 0
- output 3: float32 [4, 4, 1000, 4000], P('dp', 'pp'), parts along dimension 0
- output 4: float32 [4, 4, 4000], P('dp', 'pp'), parts along dimension 0
- output 5: float32 [4, 4, 256, 1000], P('dp', 'pp'), parts along dimension 0
- output 6: float32 [4, 4, 256, 1000], P('dp', 'pp'), parts along dimension 0
There are 2 independent parts. The reference program is written for one: setup_inputs(seed, part) draws one part's arguments, and reference() takes and returns one part's arrays. A program takes and returns all parts, laid end to end along the dimension named above; each array names one.
All inputs are finite; a program needn't handle non-finite values.
Results may differ from the reference program's by a relative error of at most 0.00973023.
Values are sent between devices in bfloat16 or wider.
A program may use at most 1 GiB of HBM per device.

```python
import jax
import jax.numpy as jnp
from jax import lax

STAGES = 4
BATCH = 256
STEPS = 32
HIDDEN = 1000
LAYERS = 2 * STAGES


def setup_inputs(seed: int = 0, part: int = 0) -> dict:
    base_key = jax.random.fold_in(jax.random.key(seed), part)
    key_list = jax.random.split(base_key, 7)
    layer_depth = (jnp.arange(2)[:, None] * STAGES + jnp.arange(STAGES)[None, :]).astype(jnp.float32)
    in_scale = (HIDDEN * (1.0 + layer_depth / 4.0)) ** -0.5
    forget_bias = jnp.where(jnp.arange(4 * HIDDEN) // HIDDEN == 1, 1.0, 0.0)
    inputs = jax.random.normal(key_list[0], (BATCH, STEPS, HIDDEN), jnp.float32)
    targets = jax.random.normal(key_list[1], (BATCH, STEPS, HIDDEN), jnp.float32)
    w_in = jax.random.normal(key_list[2], (2, STAGES, HIDDEN, 4 * HIDDEN), jnp.float32) * in_scale[:, :, None, None]
    w_hid = jax.random.normal(key_list[3], (2, STAGES, HIDDEN, 4 * HIDDEN), jnp.float32) * HIDDEN ** -0.5
    bias = 0.5 * jax.random.normal(key_list[4], (2, STAGES, 4 * HIDDEN), jnp.float32) + forget_bias
    h_init = 0.5 * jax.random.normal(key_list[5], (2, STAGES, BATCH, HIDDEN), jnp.float32)
    c_init = jax.random.normal(key_list[6], (2, STAGES, BATCH, HIDDEN), jnp.float32)
    return {'inputs': inputs.astype(jnp.bfloat16), 'targets': targets.astype(jnp.bfloat16), 'w_in': w_in.astype(jnp.bfloat16), 'w_hid': w_hid.astype(jnp.bfloat16), 'bias': bias, 'h_init': h_init, 'c_init': c_init}


def cell_step(proj_t, h_prev, c_prev, w_hid, bias_row):
    n_hidden = c_prev.shape[-1]
    pre_act = proj_t + jnp.dot(h_prev, w_hid, preferred_element_type=jnp.float32) + bias_row
    gate_i = jax.nn.sigmoid(pre_act[:, :n_hidden])
    gate_f = jax.nn.sigmoid(pre_act[:, n_hidden:2 * n_hidden])
    gate_g = jnp.tanh(pre_act[:, 2 * n_hidden:3 * n_hidden])
    gate_o = jax.nn.sigmoid(pre_act[:, 3 * n_hidden:])
    c_new = gate_f * c_prev + gate_i * gate_g
    h_new = (gate_o * jnp.tanh(c_new)).astype(jnp.bfloat16)
    return pre_act, c_new, h_new


def cell_grad(pre_act, c_prev, c_now, dh_total, dc_carry):
    n_hidden = c_now.shape[-1]
    gate_i = jax.nn.sigmoid(pre_act[:, :n_hidden])
    gate_f = jax.nn.sigmoid(pre_act[:, n_hidden:2 * n_hidden])
    gate_g = jnp.tanh(pre_act[:, 2 * n_hidden:3 * n_hidden])
    gate_o = jax.nn.sigmoid(pre_act[:, 3 * n_hidden:])
    tanh_c = jnp.tanh(c_now)
    dc_total = dc_carry + dh_total * gate_o * (1.0 - tanh_c * tanh_c)
    grad_pre = jnp.concatenate([dc_total * gate_g * gate_i * (1.0 - gate_i), dc_total * c_prev * gate_f * (1.0 - gate_f), dc_total * gate_i * (1.0 - gate_g * gate_g), dh_total * tanh_c * gate_o * (1.0 - gate_o)], axis=-1)
    return grad_pre, dc_total * gate_f


def layer_forward(seq_in, w_in, w_hid, bias_row, h_first, c_first):
    projected = jnp.einsum('tbh,hg->tbg', seq_in.astype(jnp.float32), w_in.astype(jnp.float32))

    def step_fn(carry, proj_t):
        h_prev, c_prev = carry
        pre_act, c_new, h_new = cell_step(proj_t, h_prev, c_prev, w_hid, bias_row)
        return (h_new, c_new), (pre_act, c_new, h_new)

    _, (pre_seq, cell_seq, h_seq) = lax.scan(step_fn, (h_first.astype(jnp.bfloat16), c_first), projected)
    out_seq = (seq_in.astype(jnp.float32) + h_seq.astype(jnp.float32)).astype(jnp.bfloat16)
    return pre_seq, cell_seq, h_seq, out_seq


def layer_backward(seq_in, w_in, w_hid, h_first, c_first, pre_seq, cell_seq, h_seq, grad_seq):
    c_prevs = jnp.concatenate([c_first[None], cell_seq[:-1]], axis=0)
    h_prevs = jnp.concatenate([h_first.astype(jnp.bfloat16)[None], h_seq[:-1]], axis=0)

    def step_fn(carry, xs_t):
        dh_last, dc_last, bias_acc = carry
        pre_t, c_prev_t, c_now_t, grad_t = xs_t
        grad_pre, dc_new = cell_grad(pre_t, c_prev_t, c_now_t, grad_t + dh_last, dc_last)
        grad_low = grad_pre.astype(jnp.bfloat16)
        dh_new = jnp.dot(grad_low, jnp.transpose(w_hid), preferred_element_type=jnp.float32)
        return (dh_new, dc_new, bias_acc + jnp.sum(grad_pre, axis=0)), grad_low

    zeros_state = jnp.zeros(c_first.shape, jnp.float32)
    bias_zero = jnp.zeros((w_hid.shape[1],), jnp.float32)
    (dh_end, dc_end, grad_bias), grad_low_seq = lax.scan(step_fn, (zeros_state, zeros_state, bias_zero), (pre_seq, c_prevs, cell_seq, grad_seq), reverse=True)
    grad_wide = grad_low_seq.astype(jnp.float32)
    grad_w_in = jnp.einsum('tbh,tbg->hg', seq_in.astype(jnp.float32), grad_wide)
    grad_w_hid = jnp.einsum('tbh,tbg->hg', h_prevs.astype(jnp.float32), grad_wide)
    grad_in = (grad_seq + jnp.einsum('tbg,hg->tbh', grad_wide, w_in.astype(jnp.float32))).astype(jnp.bfloat16)
    return grad_in, grad_w_in, grad_w_hid, grad_bias, dh_end, dc_end


def reference(inputs, targets, w_in, w_hid, bias, h_init, c_init):
    wx_all = w_in.reshape(LAYERS, HIDDEN, 4 * HIDDEN)
    wh_all = w_hid.reshape(LAYERS, HIDDEN, 4 * HIDDEN)
    bias_all = bias.reshape(LAYERS, 4 * HIDDEN)
    h_all = h_init.reshape(LAYERS, BATCH, HIDDEN)
    c_all = c_init.reshape(LAYERS, BATCH, HIDDEN)
    seq_first = jnp.swapaxes(inputs, 0, 1)

    def fwd_body(seq_in, layer_args):
        w_x, w_h, bias_row, h_first, c_first = layer_args
        out_seq = layer_forward(seq_in, w_x, w_h, bias_row, h_first, c_first)[3]
        return out_seq, seq_in

    top_seq, layer_inputs = lax.scan(fwd_body, seq_first, (wx_all, wh_all, bias_all, h_all, c_all))
    inv_count = 1.0 / (BATCH * STEPS)
    error_seq = top_seq.astype(jnp.float32) - jnp.swapaxes(targets, 0, 1).astype(jnp.float32)
    loss = 0.5 * inv_count * jnp.sum(error_seq * error_seq)

    def bwd_body(grad_seq, layer_args):
        seq_in, w_x, w_h, bias_row, h_first, c_first = layer_args
        pre_seq, cell_seq, h_seq, _ = layer_forward(seq_in, w_x, w_h, bias_row, h_first, c_first)
        grad_in, grad_wx, grad_wh, grad_b, dh_end, dc_end = layer_backward(seq_in, w_x, w_h, h_first, c_first, pre_seq, cell_seq, h_seq, grad_seq)
        return grad_in.astype(jnp.float32), (grad_wx, grad_wh, grad_b, dh_end, dc_end)

    _, grads = lax.scan(bwd_body, error_seq * inv_count, (layer_inputs, wx_all, wh_all, bias_all, h_all, c_all), reverse=True)
    grad_wx_all, grad_wh_all, grad_b_all, grad_h_all, grad_c_all = grads
    return (loss.reshape(1), grad_wx_all.reshape(2, STAGES, HIDDEN, 4 * HIDDEN), grad_wh_all.reshape(2, STAGES, HIDDEN, 4 * HIDDEN), grad_b_all.reshape(2, STAGES, 4 * HIDDEN), grad_h_all.reshape(2, STAGES, BATCH, HIDDEN), grad_c_all.reshape(2, STAGES, BATCH, HIDDEN))
```

```python
import functools

import jax
import jax.numpy as jnp
from jax import lax
from jax.experimental import pallas as pl
from jax.experimental.pallas import tpu as pltpu
from jax.sharding import PartitionSpec as P

F32 = jnp.float32
BF16 = jnp.bfloat16
MESH = pl.DeviceIdType.MESH
BLK = 256
ROWS = 16
VMEM_LIMIT = 67043328


def _sigmoid(v):
    return 0.5 * jnp.tanh(0.5 * v) + 0.5


def _enter(n_stages):
    stage = lax.axis_index('pp')
    nxt = lax.rem(stage + 1, n_stages)
    prv = lax.rem(stage + n_stages - 1, n_stages)
    barrier = pltpu.get_barrier_semaphore()
    for peer in (nxt, prv):
        pl.semaphore_signal(barrier, inc=1, device_id={'pp': peer}, device_id_type=MESH)
    pl.semaphore_wait(barrier, 2)
    return stage, nxt, prv


def _fwd_kernel(n_stages, n_steps, n_blk, seq0, wx_hbm, wh_hbm, bias, h0, c0, landing, r_t, h_t, gates, cells, top, wx, wh, xb0, xb1, hb0, hb1, cb0, cb1, gb0, gb1, ob0, ob1, xt0, xt1, ht0, ht1, w_sem, x_sem, g_sem, c_sem, o_sem, xt_sem, ht_sem, i_sem, recv_sem):
    stage, nxt, _ = _enter(n_stages)
    n_total = 2 * n_steps
    xb, hb, cb, gb, ob = (xb0, xb1), (hb0, hb1), (cb0, cb1), (gb0, gb1), (ob0, ob1)
    xt, ht = (xt0, xt1), (ht0, ht1)
    is_first = stage == 0
    is_last = stage == n_stages - 1

    def weight_copies(k):
        return [pltpu.make_async_copy(wx_hbm.at[k], wx.at[k], w_sem.at[2 * k]), pltpu.make_async_copy(wh_hbm.at[k], wh.at[k], w_sem.at[2 * k + 1])]

    for k in range(2):
        for copy in weight_copies(k):
            copy.start()

    def landed(n):
        k, t = n // n_steps, lax.rem(n, n_steps)
        return pltpu.make_async_remote_copy(src_ref=ob0, dst_ref=landing.at[k, t], send_sem=o_sem.at[0, 0], recv_sem=recv_sem.at[n], device_id={'pp': nxt}, device_id_type=MESH)

    def fetch(n, u):
        k, t = n // n_steps, lax.rem(n, n_steps)
        from_args = is_first & (k == 0)

        @pl.when(from_args)
        def _():
            pltpu.make_async_copy(seq0.at[t], xb[u], x_sem.at[u]).start()

        @pl.when(jnp.logical_not(from_args))
        def _():
            landed(n).wait_recv()
            pltpu.make_async_copy(landing.at[k, t], xb[u], x_sem.at[u]).start()

    def cols(j):
        return pl.ds(j * BLK, BLK)

    def send(n, u, j):
        k, t = n // n_steps, lax.rem(n, n_steps)
        k_next = jnp.minimum(k + stage // (n_stages - 1), 1)
        return pltpu.make_async_remote_copy(src_ref=ob[u].at[:, cols(j)], dst_ref=landing.at[k_next, t, :, cols(j)], send_sem=o_sem.at[u, j], recv_sem=recv_sem.at[k_next * n_steps + t], device_id={'pp': nxt}, device_id_type=MESH)

    def keep(n, u, j):
        return pltpu.make_async_copy(ob[u].at[:, cols(j)], top.at[lax.rem(n, n_steps), :, cols(j)], o_sem.at[u, j])

    def cell_copy(n, u):
        return pltpu.make_async_copy(cb[u], cells.at[n // n_steps, lax.rem(n, n_steps) + 1], c_sem.at[u])

    def out_copies(n, u):
        k, t = n // n_steps, lax.rem(n, n_steps)
        return [pltpu.make_async_copy(gb[u].at[j], gates.at[k, t, j], g_sem.at[u, j]) for j in range(n_blk)] + [cell_copy(n, u), pltpu.make_async_copy(xt[u], r_t.at[k, t], xt_sem.at[u]), pltpu.make_async_copy(ht[u], h_t.at[k, t], ht_sem.at[u])]

    def wait_outs(n, u):
        for copy in out_copies(n, u):
            copy.wait()
        at_top = is_last & (n // n_steps == 1)

        @pl.when(at_top)
        def _():
            for j in range(n_blk):
                keep(n, u, j).wait()

        @pl.when(jnp.logical_not(at_top))
        def _():
            for j in range(n_blk):
                send(n, u, j).wait_send()

    fetch(0, 0)

    def step(n, u):
        k, t = n // n_steps, lax.rem(n, n_steps)
        v = 1 - u
        if u == 0:

            @pl.when(t == 0)
            def _():
                for copy in weight_copies(k):
                    copy.wait()

                @pl.when(n > 0)
                def _():
                    cell_copy(n - 1, v).wait()

                h_in = pltpu.make_async_copy(h0.at[k], hb[v], i_sem.at[0])
                c_in = pltpu.make_async_copy(c0.at[k], cb[v], i_sem.at[1])
                h_in.start()
                c_in.start()
                h_in.wait()
                c_in.wait()
                pltpu.make_async_copy(cb[v], cells.at[k, 0], c_sem.at[v]).start()

        else:

            @pl.when(n == 1)
            def _():
                cell_copy(n, u).wait()

        @pl.when(n >= 2)
        def _():
            wait_outs(n - 2, u)

        pltpu.make_async_copy(seq0.at[0], xb[u], x_sem.at[u]).wait()
        for j in range(n_blk):
            z = jnp.dot(xb[u][...], wx[k, j], preferred_element_type=F32) + jnp.dot(hb[v][...], wh[k, j], preferred_element_type=F32)
            gb[u][j] = z + bias[k, j]
            for r in range(0, BLK, ROWS):
                rows = pl.ds(r, ROWS)
                gate_i = _sigmoid(gb[u][j, rows, 0:BLK])
                gate_f = _sigmoid(gb[u][j, rows, BLK:2 * BLK])
                gate_g = jnp.tanh(gb[u][j, rows, 2 * BLK:3 * BLK])
                gate_o = _sigmoid(gb[u][j, rows, 3 * BLK:4 * BLK])
                c_new = gate_f * cb[v][rows, cols(j)] + gate_i * gate_g
                h_new = (gate_o * jnp.tanh(c_new)).astype(BF16)
                gb[u][j, rows, 0:BLK] = gate_i
                gb[u][j, rows, BLK:2 * BLK] = gate_f
                gb[u][j, rows, 2 * BLK:3 * BLK] = gate_g
                gb[u][j, rows, 3 * BLK:4 * BLK] = gate_o
                cb[u][rows, cols(j)] = c_new
                hb[u][rows, cols(j)] = h_new
                ob[u][rows, cols(j)] = (xb[u][rows, cols(j)].astype(F32) + h_new.astype(F32)).astype(BF16)
            xt[u][cols(j), :] = xb[u][:, cols(j)].T
            ht[u][cols(j), :] = hb[v][:, cols(j)].T
            if j == n_blk - 2:

                @pl.when(n + 1 < n_total)
                def _():
                    fetch(n + 1, v)

        at_top = is_last & (k == 1)

        @pl.when(at_top)
        def _():
            for j in range(n_blk):
                keep(n, u, j).start()

        @pl.when(jnp.logical_not(at_top))
        def _():
            for j in range(n_blk):
                send(n, u, j).start()

        for copy in out_copies(n, u):
            copy.start()

    def pair(i, carry):
        step(2 * i, 0)
        step(2 * i + 1, 1)
        return carry

    lax.fori_loop(0, n_steps, pair, 0)
    wait_outs(n_total - 2, 0)
    wait_outs(n_total - 1, 1)


def _bwd_kernel(n_stages, n_steps, n_blk, scale, gates, cells, h_t, top, target, wx_hbm, wh_hbm, landing, dz_seq, dwh, db, dh_out, dc_out, loss, wx, wh, acc, zb0, zb1, gb0, gb1, cb0, cb1, ab0, ab1, tb0, tb1, ob0, ob1, hb0, hb1, dh, dc, bacc, lacc, w_sem, g_sem, c_sem, a_sem, t_sem, h_sem, z_sem, o_sem, f_sem, recv_sem):
    stage, nxt, prv = _enter(n_stages)
    n_total = 2 * n_steps
    zb, gb, cb, ab, tb, ob, hb = (zb0, zb1), (gb0, gb1), (cb0, cb1), (ab0, ab1), (tb0, tb1), (ob0, ob1), (hb0, hb1)
    is_first = stage == 0
    is_last = stage == n_stages - 1

    def weight_copies(k):
        return [pltpu.make_async_copy(wx_hbm.at[k], wx, w_sem.at[0]), pltpu.make_async_copy(wh_hbm.at[k], wh, w_sem.at[1])]

    for copy in weight_copies(1):
        copy.start()

    def place(n):
        return 1 - n // n_steps, n_steps - 1 - lax.rem(n, n_steps)

    def cols(j):
        return pl.ds(j * BLK, BLK)

    def landed(n):
        k, t = place(n)
        return pltpu.make_async_remote_copy(src_ref=ob0, dst_ref=landing.at[k, t], send_sem=o_sem.at[0, 0], recv_sem=recv_sem.at[n], device_id={'pp': prv}, device_id_type=MESH)

    def fetch_saved(n, u):
        k, t = place(n)
        for j in range(n_blk):
            pltpu.make_async_copy(gates.at[k, t, j], gb[u].at[j], g_sem.at[u, j]).start()
        pltpu.make_async_copy(cells.at[k, pl.ds(t, 2)], cb[u], c_sem.at[u]).start()
        pltpu.make_async_copy(h_t.at[k, t], hb[u], h_sem.at[u]).start()

    def wait_saved(u):
        for j in range(n_blk):
            pltpu.make_async_copy(gates.at[0, 0, j], gb[u].at[j], g_sem.at[u, j]).wait()
        pltpu.make_async_copy(cells.at[0, pl.ds(0, 2)], cb[u], c_sem.at[u]).wait()

    def wait_h(u):
        pltpu.make_async_copy(h_t.at[0, 0], hb[u], h_sem.at[u]).wait()

    def fetch_grad(n, u):
        k, t = place(n)
        at_top = is_last & (k == 1)

        @pl.when(at_top)
        def _():
            pltpu.make_async_copy(top.at[t], ab[u], a_sem.at[u]).start()
            pltpu.make_async_copy(target.at[t], tb[u], t_sem.at[u]).start()

        @pl.when(jnp.logical_not(at_top))
        def _():
            landed(n).wait_recv()
            pltpu.make_async_copy(landing.at[k, t], ab[u], a_sem.at[u]).start()

    def wait_grad(n, u):
        pltpu.make_async_copy(top.at[0], ab[u], a_sem.at[u]).wait()

        @pl.when(is_last & (n // n_steps == 0))
        def _():
            pltpu.make_async_copy(target.at[0], tb[u], t_sem.at[u]).wait()

    def send(n, u, j):
        k, t = place(n)
        k_next = jnp.maximum(k - (n_stages - 1 - stage) // (n_stages - 1), 0)
        n_next = (1 - k_next) * n_steps + lax.rem(n, n_steps)
        return pltpu.make_async_remote_copy(src_ref=ob[u].at[:, cols(j)], dst_ref=landing.at[k_next, t, :, cols(j)], send_sem=o_sem.at[u, j], recv_sem=recv_sem.at[n_next], device_id={'pp': prv}, device_id_type=MESH)

    def sends(n):
        return jnp.logical_not(is_first & (n // n_steps == 1))

    def dz_copies(n, u):
        k, t = place(n)
        return [pltpu.make_async_copy(zb[u].at[j], dz_seq.at[k, t, j], z_sem.at[u, j]) for j in range(n_blk)]

    def wait_outs(n, u):
        for copy in dz_copies(n, u):
            copy.wait()

        @pl.when(sends(n))
        def _():
            for j in range(n_blk):
                send(n, u, j).wait_send()

    def weight_grad(v, j):
        acc[j] += jnp.dot(hb[v][...], zb[v][j], preferred_element_type=F32)

    acc_copies = lambda k: [pltpu.make_async_copy(acc, dwh.at[k], f_sem.at[0]), pltpu.make_async_copy(dh, dh_out.at[k], f_sem.at[1]), pltpu.make_async_copy(dc, dc_out.at[k], f_sem.at[2]), pltpu.make_async_copy(bacc, db.at[k], f_sem.at[3])]

    def begin_round():
        acc[...] = jnp.zeros_like(acc)
        dh[...] = jnp.zeros_like(dh)
        dc[...] = jnp.zeros_like(dc)
        bacc[...] = jnp.zeros_like(bacc)
        tb0[...] = jnp.zeros_like(tb0)
        tb1[...] = jnp.zeros_like(tb1)
        zb1[...] = jnp.zeros_like(zb1)

    def end_round(k, n_last):
        wait_h(1)
        for j in range(n_blk):
            weight_grad(1, j)
        for copy in acc_copies(k):
            copy.start()
        for copy in acc_copies(k):
            copy.wait()

    begin_round()
    lacc[...] = jnp.zeros_like(lacc)
    fetch_saved(0, 0)
    fetch_grad(0, 0)
    hb1[...] = jnp.zeros_like(hb1)
    for copy in weight_copies(1):
        copy.wait()

    def step(n, u):
        k, t = place(n)
        v = 1 - u
        if u == 0:

            @pl.when(n == n_steps)
            def _():
                wait_h(1)
                for j in range(n_blk):
                    weight_grad(1, j)
                for copy in weight_copies(0):
                    copy.start()
                wait_outs(n - 1, 1)
                for copy in acc_copies(1):
                    copy.start()
                for copy in acc_copies(1):
                    copy.wait()
                begin_round()
                hb1[...] = jnp.zeros_like(hb1)
                for copy in weight_copies(0):
                    copy.wait()

        if u == 0:

            @pl.when((n >= 2) & (n != n_steps))
            def _():
                wait_h(v)
                wait_outs(n - 2, u)

            @pl.when(n == n_steps)
            def _():
                wait_outs(n - 2, u)
        else:
            wait_h(v)

            @pl.when((n >= 2) & (n != n_steps + 1))
            def _():
                wait_outs(n - 2, u)

            @pl.when(n == n_steps + 1)
            def _():
                pass

        wait_saved(u)
        wait_grad(n, u)
        mult = jnp.where(is_last & (k == 1), scale, 1.0).astype(F32)
        for j in range(n_blk):
            weight_grad(v, j)
            for r in range(0, BLK, ROWS):
                rows = pl.ds(r, ROWS)
                gate_i = gb[u][j, rows, 0:BLK]
                gate_f = gb[u][j, rows, BLK:2 * BLK]
                gate_g = gb[u][j, rows, 2 * BLK:3 * BLK]
                gate_o = gb[u][j, rows, 3 * BLK:4 * BLK]
                c_prev = cb[u][0, rows, cols(j)]
                tanh_c = jnp.tanh(cb[u][1, rows, cols(j)])
                diff = ab[u][rows, cols(j)].astype(F32) - tb[u][rows, cols(j)].astype(F32)
                lacc[:, cols(j)] += diff[0:8] * diff[0:8] + diff[8:16] * diff[8:16]
                dh_all = diff * mult + dh[rows, cols(j)]
                dho = dh_all * gate_o
                dc_all = dc[rows, cols(j)] + dho * (1.0 - tanh_c * tanh_c)
                dz_i = dc_all * gate_g * gate_i * (1.0 - gate_i)
                dz_f = dc_all * c_prev * gate_f * (1.0 - gate_f)
                dz_g = dc_all * gate_i * (1.0 - gate_g * gate_g)
                dz_o = dho * tanh_c * (1.0 - gate_o)
                dc[rows, cols(j)] = dc_all * gate_f
                for g, dz in enumerate((dz_i, dz_f, dz_g, dz_o)):
                    bacc[j, :, g * BLK:(g + 1) * BLK] += dz[0:8] + dz[8:16]
                    zb[u][j, rows, g * BLK:(g + 1) * BLK] = dz.astype(BF16)
        for copy in dz_copies(n, u):
            copy.start()
        contract = (((1,), (1,)), ((), ()))
        for i in range(n_blk):
            dh[:, cols(i)] = sum(lax.dot_general(zb[u][j], wh[j, cols(i), :], contract, preferred_element_type=F32) for j in range(n_blk))

        @pl.when(n + 1 < n_total)
        def _():
            fetch_saved(n + 1, v)
            fetch_grad(n + 1, v)

        for i in range(n_blk):
            part = sum(lax.dot_general(zb[u][j], wx[j, cols(i), :], contract, preferred_element_type=F32) for j in range(n_blk))
            into = (ab[u][:, cols(i)].astype(F32) - tb[u][:, cols(i)].astype(F32)) * mult
            ob[u][:, cols(i)] = (into + part).astype(BF16)

        @pl.when(sends(n))
        def _():
            for i in range(n_blk):
                send(n, u, i).start()

        @pl.when(n == n_steps - 1)
        def _():
            out = pltpu.make_async_copy(lacc, loss, f_sem.at[0])
            out.start()
            out.wait()

    def pair(i, carry):
        step(2 * i, 0)
        step(2 * i + 1, 1)
        return carry

    lax.fori_loop(0, n_steps, pair, 0)
    wait_outs(n_total - 2, 0)
    wait_outs(n_total - 1, 1)
    end_round(0, n_total - 1)


def _natural(n_hid, n_blk, src, dst):
    for g in range(4):
        for j in range(n_blk):
            width = min(BLK, n_hid - j * BLK)
            dst[:, g * n_hid + j * BLK:g * n_hid + j * BLK + width] = src(j, g)[:, :width]


def _dense_kernel(n_hid, n_blk, n_chunk, r_ref, z_ref, packed_ref, dwx_ref, dwh_ref, acc):
    chunk = pl.program_id(2)

    @pl.when(chunk == 0)
    def _():
        acc[...] = jnp.zeros_like(acc)

    for j in range(n_blk):
        acc[j] += sum(jnp.dot(r_ref[0, t], z_ref[0, t, j], preferred_element_type=F32) for t in range(n_chunk))
    _natural(n_hid, n_blk, lambda j, g: packed_ref[0, j, :, g * BLK:(g + 1) * BLK], dwh_ref.at[0])

    @pl.when(chunk == pl.num_programs(2) - 1)
    def _():
        _natural(n_hid, n_blk, lambda j, g: acc[j, :, g * BLK:(g + 1) * BLK], dwx_ref.at[0])


def solution(mesh):
    n_stages = mesh.shape['pp']

    def local_fn(inputs, targets, w_in, w_hid, bias, h_init, c_init):
        n_batch, n_steps, n_hid = inputs.shape
        n_blk = -(-n_hid // BLK)
        n_pad = n_blk * BLK
        extra = n_pad - n_hid
        stage = lax.axis_index('pp')

        def time_major(seq):
            return jnp.pad(jnp.swapaxes(seq, 0, 1), ((0, 0), (0, 0), (0, extra)))

        def pack(w):
            lead, rows = w.shape[0], w.shape[1]
            parts = jnp.pad(w.reshape(lead, rows, 4, n_hid), ((0, 0), (0, (-rows) % BLK if rows > 1 else 0), (0, 0), (0, extra)))
            parts = parts.reshape(lead, parts.shape[1], 4, n_blk, BLK)
            return jnp.transpose(parts, (0, 3, 1, 2, 4)).reshape(lead, n_blk, parts.shape[1], 4 * BLK)

        seq0 = time_major(inputs)
        target = time_major(targets)
        wx_p, wh_p = pack(w_in[:, 0]), pack(w_hid[:, 0])
        bias_p = pack(bias)
        h0 = jnp.pad(h_init[:, 0], ((0, 0), (0, 0), (0, extra))).astype(BF16)
        c0 = jnp.pad(c_init[:, 0], ((0, 0), (0, 0), (0, extra)))

        def shape(*dims, dtype=BF16):
            return jax.ShapeDtypeStruct(dims, dtype)

        any_spec = pl.BlockSpec(memory_space=pl.ANY)
        vmem_spec = pl.BlockSpec(memory_space=pltpu.VMEM)
        row = (n_batch, n_pad)
        dma = pltpu.SemaphoreType.DMA
        step_flops = 2 * n_batch * n_pad * 4 * n_pad
        _, r_t, h_t, gates, cells, top = pl.pallas_call(
            functools.partial(_fwd_kernel, n_stages, n_steps, n_blk),
            out_shape=(shape(2, n_steps, *row), shape(2, n_steps, n_pad, n_batch), shape(2, n_steps, n_pad, n_batch), shape(2, n_steps, n_blk, n_batch, 4 * BLK, dtype=F32), shape(2, n_steps + 1, *row, dtype=F32), shape(n_steps, *row)),
            in_specs=[any_spec, any_spec, any_spec, vmem_spec, any_spec, any_spec],
            out_specs=[any_spec] * 6,
            scratch_shapes=[pltpu.VMEM((2, n_blk, n_pad, 4 * BLK), BF16)] * 2 + [pltpu.VMEM(row, BF16)] * 4 + [pltpu.VMEM(row, F32)] * 2 + [pltpu.VMEM((n_blk, n_batch, 4 * BLK), F32)] * 2 + [pltpu.VMEM(row, BF16)] * 2 + [pltpu.VMEM((n_pad, n_batch), BF16)] * 4 + [dma((4,)), dma((2,)), dma((2, n_blk)), dma((2,)), dma((2, n_blk)), dma((2,)), dma((2,)), dma((2,)), dma((2 * n_steps,))],
            compiler_params=pltpu.CompilerParams(collective_id=0, has_side_effects=True, vmem_limit_bytes=VMEM_LIMIT),
            cost_estimate=pl.CostEstimate(flops=4 * n_steps * step_flops, bytes_accessed=0, transcendentals=0),
            name='lstm_forward',
        )(seq0, wx_p, wh_p, bias_p, h0, c0)

        scale = 1.0 / (n_batch * n_steps)
        _, dz_seq, dwh_p, db_p, dh_p, dc_p, loss_p = pl.pallas_call(
            functools.partial(_bwd_kernel, n_stages, n_steps, n_blk, scale),
            out_shape=(shape(2, n_steps, *row), shape(2, n_steps, n_blk, n_batch, 4 * BLK), shape(2, n_blk, n_pad, 4 * BLK, dtype=F32), shape(2, n_blk, 8, 4 * BLK, dtype=F32), shape(2, *row, dtype=F32), shape(2, *row, dtype=F32), shape(8, n_pad, dtype=F32)),
            in_specs=[any_spec] * 7,
            out_specs=[any_spec] * 7,
            scratch_shapes=[pltpu.VMEM((n_blk, n_pad, 4 * BLK), BF16)] * 2 + [pltpu.VMEM((n_blk, n_pad, 4 * BLK), F32)] + [pltpu.VMEM((n_blk, n_batch, 4 * BLK), BF16)] * 2 + [pltpu.VMEM((n_blk, n_batch, 4 * BLK), F32)] * 2 + [pltpu.VMEM((2, *row), F32)] * 2 + [pltpu.VMEM(row, BF16)] * 6 + [pltpu.VMEM((n_pad, n_batch), BF16)] * 2 + [pltpu.VMEM(row, F32)] * 2 + [pltpu.VMEM((n_blk, 8, 4 * BLK), F32), pltpu.VMEM((8, n_pad), F32)] + [dma((2,)), dma((2, n_blk)), dma((2,)), dma((2,)), dma((2,)), dma((2,)), dma((2, n_blk)), dma((2, n_blk)), dma((4,)), dma((2 * n_steps,))],
            compiler_params=pltpu.CompilerParams(collective_id=1, has_side_effects=True, vmem_limit_bytes=VMEM_LIMIT),
            cost_estimate=pl.CostEstimate(flops=6 * n_steps * step_flops, bytes_accessed=0, transcendentals=0),
            name='lstm_backward',
        )(gates, cells, h_t, top, target, wx_p, wh_p)

        n_chunk = 4
        m_rows = 512
        m_tiles = n_pad // m_rows
        per_round = m_tiles * (n_steps // n_chunk)
        p_rows = n_pad // per_round
        part = lambda k, m, c: m * (n_steps // n_chunk) + c
        dwx, dwh = pl.pallas_call(
            functools.partial(_dense_kernel, n_hid, n_blk, n_chunk),
            grid=(2, m_tiles, n_steps // n_chunk),
            out_shape=(shape(2, n_hid, 4 * n_hid, dtype=F32), shape(2, n_hid, 4 * n_hid, dtype=F32)),
            in_specs=[pl.BlockSpec((1, n_chunk, m_rows, n_batch), lambda k, m, c: (k, c, m, 0)), pl.BlockSpec((1, n_chunk, n_blk, n_batch, 4 * BLK), lambda k, m, c: (k, c, 0, 0, 0)), pl.BlockSpec((1, n_blk, p_rows, 4 * BLK), lambda k, m, c: (k, 0, part(k, m, c), 0))],
            out_specs=[pl.BlockSpec((1, m_rows, 4 * n_hid), lambda k, m, c: (k, m, 0)), pl.BlockSpec((1, p_rows, 4 * n_hid), lambda k, m, c: (k, part(k, m, c), 0))],
            scratch_shapes=[pltpu.VMEM((n_blk, m_rows, 4 * BLK), F32)],
            compiler_params=pltpu.CompilerParams(dimension_semantics=('arbitrary', 'arbitrary', 'arbitrary'), vmem_limit_bytes=VMEM_LIMIT),
            cost_estimate=pl.CostEstimate(flops=2 * n_steps * step_flops, bytes_accessed=0, transcendentals=0),
            name='input_weight_grad',
        )(r_t, dz_seq, dwh_p)

        local_loss = jnp.where(stage == n_stages - 1, 0.5 * scale * jnp.sum(loss_p), 0.0)
        loss = lax.psum(local_loss, 'pp')
        db = jnp.sum(db_p, axis=2).reshape(2, n_blk, 4, BLK)
        db = jnp.transpose(db, (0, 2, 1, 3)).reshape(2, 4, n_pad)[:, :, :n_hid].reshape(2, 4 * n_hid)
        return loss[None], dwx[:, None], dwh[:, None], db[:, None], dh_p[:, None, :, :n_hid], dc_p[:, None, :, :n_hid]

    spec_seq = P('dp', None, None)
    spec_weight = P('dp', 'pp', None, None)
    spec_bias = P('dp', 'pp', None)
    return jax.shard_map(local_fn, mesh=mesh, in_specs=(spec_seq, spec_seq, spec_weight, spec_weight, spec_bias, spec_weight, spec_weight), out_specs=(P('dp'), spec_weight, spec_weight, spec_bias, spec_weight, spec_weight), check_vma=False)
```

```python
import functools

import jax
import jax.numpy as jnp
from jax import lax
from jax.experimental import pallas as pl
from jax.experimental.pallas import tpu as pltpu
from jax.sharding import PartitionSpec as P

F32 = jnp.float32
BF16 = jnp.bfloat16
MESH = pl.DeviceIdType.MESH
LANES = 128
BLK = 256
FINE = 128
ROWS = 16
SLOTS = 4
VMEM_LIMIT = 67043328
ALONG_LANES = (((1,), (1,)), ((), ()))


def _blocks(n_hid, block=BLK):
    return [(r, min(block, n_hid - r)) for r in range(0, n_hid, block)]


def _chunks(first, count):
    return [(first + r, min(ROWS, count - r)) for r in range(0, count, ROWS)]


def _segments(n_hid, first, count):
    runs, n = [], first
    while n < first + count:
        gate, hid = n // n_hid, n % n_hid
        base = hid // FINE * FINE
        size = min(FINE, n_hid - base)
        length = min(first + count - n, base + size - hid)
        runs.append((n - first, length, 4 * base + gate * size + hid - base, gate))
        n += length
    return runs


def _enter(n_stages):
    stage = lax.axis_index('pp')
    nxt = lax.rem(stage + 1, n_stages)
    prv = lax.rem(stage + n_stages - 1, n_stages)
    barrier = pltpu.get_barrier_semaphore()
    for peer in (nxt, prv):
        pl.semaphore_signal(barrier, inc=1, device_id={'pp': peer}, device_id_type=MESH)
    pl.semaphore_wait(barrier, 2)
    return stage, nxt, prv


def _fwd_kernel(n_stages, n_steps, n_hid, seq0, wx_hbm, wh_hbm, bias_in, h0, c0, wrap, r_seq, h_seq, saved, top, wt, stage_buf, eye, bias, ring, hb0, hb1, cell, zb0, zb1, fb0, fb1, ob, w_sem, x_sem, r_sem, f_sem, h_sem, o_sem, i_sem, recv_sem, wrap_sem, free_sem):
    n_total = 2 * n_steps
    n_gate = 4 * n_hid
    n_pad = wt.shape[-1]
    blocks = _blocks(n_hid, FINE)
    parts = _blocks(n_hid)
    hb, fb, zb = (hb0, hb1), (fb0, fb1), (zb0, zb1)
    valid = pl.ds(0, n_hid)
    n_cut = n_pad // BLK
    tail = n_hid - (n_cut - 1) * BLK
    halved = (0.5, 0.5, 1.0, 0.5)

    def unit_copies(k, m, act):
        mat, cut = m // n_cut, lax.rem(m, n_cut)
        slot = lax.rem(m, 2)
        for which, src in enumerate((wx_hbm, wh_hbm)):

            @pl.when((mat == which) & (cut < n_cut - 1))
            def _(src=src):
                act(pltpu.make_async_copy(src.at[k, pl.ds(pl.multiple_of(cut * BLK, BLK), BLK)], stage_buf.at[slot], w_sem.at[slot]))

            @pl.when((mat == which) & (cut == n_cut - 1))
            def _(src=src):
                act(pltpu.make_async_copy(src.at[k, pl.ds((n_cut - 1) * BLK, tail)], stage_buf.at[slot, pl.ds(0, tail)], w_sem.at[slot]))

    def transpose_unit(k, m):
        mat, cut = m // n_cut, lax.rem(m, n_cut)
        slot = lax.rem(m, 2)
        unit_copies(k, m, lambda copy: copy.wait())

        @pl.when(cut == n_cut - 1)
        def _():
            stage_buf[slot, tail:, :] = jnp.zeros((BLK - tail, n_gate), BF16)

        for n in range(0, n_gate, BLK):
            width = min(BLK, n_gate - n)
            tile = lax.dot_general(eye[0:width, 0:width], stage_buf[slot, :, n:n + width], ALONG_LANES, preferred_element_type=F32)
            for at, length, row, gate in _segments(n_hid, n, width):
                wt[mat, k, pl.ds(row, length), pl.ds(pl.multiple_of(cut * BLK, BLK), BLK)] = (tile[at:at + length] * halved[gate]).astype(BF16)

        @pl.when(m + 2 < 2 * n_cut)
        def _():
            unit_copies(k, m + 2, lambda copy: copy.start())

    def spread_bias(k):
        for n in range(0, n_gate, LANES):
            width = min(LANES, n_gate - n)
            tile = jnp.broadcast_to(bias_in[k, :, n:n + width], (LANES, width)).T
            for at, length, row, gate in _segments(n_hid, n, width):
                bias[row:row + length, :] = tile[at:at + length] * halved[gate]

    unit_copies(0, 0, lambda copy: copy.start())
    unit_copies(0, 1, lambda copy: copy.start())
    for buf in (hb0, hb1):
        buf[n_hid:, :] = jnp.zeros((n_pad - n_hid, buf.shape[1]), BF16)
    for s in range(SLOTS):
        ring[s, n_hid:, :] = jnp.zeros((n_pad - n_hid, ring.shape[2]), BF16)
    eye[...] = (lax.broadcasted_iota(jnp.int32, (BLK, BLK), 0) == lax.broadcasted_iota(jnp.int32, (BLK, BLK), 1)).astype(F32).astype(BF16)
    stage, nxt, prv = _enter(n_stages)
    is_first = stage == 0
    is_last = stage == n_stages - 1

    def fetch(n):
        k, t = n // n_steps, lax.rem(n, n_steps)
        slot = lax.rem(n, SLOTS)

        @pl.when(is_first & (k == 0))
        def _():
            pltpu.make_async_copy(seq0.at[t], ring.at[slot, valid], x_sem.at[slot]).start()

        @pl.when(is_first & (k == 1))
        def _():
            pltpu.make_async_remote_copy(src_ref=ob.at[0], dst_ref=wrap.at[t], send_sem=o_sem.at[0, 0], recv_sem=wrap_sem.at[t], device_id={'pp': nxt}, device_id_type=MESH).wait_recv()
            pltpu.make_async_copy(wrap.at[t], ring.at[slot, valid], x_sem.at[slot]).start()

    def arrive(n):
        slot = lax.rem(n, SLOTS)

        @pl.when(is_first)
        def _():
            pltpu.make_async_copy(seq0.at[0], ring.at[slot, valid], x_sem.at[slot]).wait()

        @pl.when(jnp.logical_not(is_first))
        def _():
            pltpu.make_async_remote_copy(src_ref=ob.at[0], dst_ref=ring.at[slot, valid], send_sem=o_sem.at[0, 0], recv_sem=recv_sem.at[slot], device_id={'pp': nxt}, device_id_type=MESH).wait_recv()

    def store_x(n):
        slot = lax.rem(n, SLOTS)
        return pltpu.make_async_copy(ring.at[slot, valid], r_seq.at[n // n_steps, lax.rem(n, n_steps)], r_sem.at[slot])

    def outgoing(n, j, act):
        k, t = n // n_steps, lax.rem(n, n_steps)
        slot = lax.rem(n, SLOTS)
        rows = pl.ds(*parts[j])

        @pl.when(jnp.logical_not(is_last))
        def _():
            act(pltpu.make_async_remote_copy(src_ref=ob.at[slot, rows], dst_ref=ring.at[slot, rows], send_sem=o_sem.at[slot, j], recv_sem=recv_sem.at[slot], device_id={'pp': nxt}, device_id_type=MESH), True)

        @pl.when(is_last & (k == 0))
        def _():
            act(pltpu.make_async_remote_copy(src_ref=ob.at[slot, rows], dst_ref=wrap.at[t, rows], send_sem=o_sem.at[slot, j], recv_sem=wrap_sem.at[t], device_id={'pp': nxt}, device_id_type=MESH), True)

        @pl.when(is_last & (k == 1))
        def _():
            act(pltpu.make_async_copy(ob.at[slot, rows], top.at[t, rows], o_sem.at[slot, j]), False)

    def start(copy, remote):
        copy.start()

    def finish(copy, remote):
        if remote:
            copy.wait_send()
        else:
            copy.wait()

    def h_copy(n, u):
        return pltpu.make_async_copy(hb[u].at[valid], h_seq.at[n // n_steps, lax.rem(n, n_steps) + 1], h_sem.at[u])

    def f_copy(n, u):
        return pltpu.make_async_copy(fb[u], saved.at[n // n_steps, lax.rem(n, n_steps)], f_sem.at[u])

    fetch(0)

    def build(m, carry):
        transpose_unit(0, m)
        return carry

    lax.fori_loop(0, 2 * n_cut, build, 0)
    unit_copies(1, 0, lambda copy: copy.start())
    unit_copies(1, 1, lambda copy: copy.start())

    def step(n, u):
        k, t = n // n_steps, lax.rem(n, n_steps)
        slot = lax.rem(n, SLOTS)
        v = 1 - u

        @pl.when((n >= 2) & (n != n_steps + 1))
        def _():
            f_copy(n - 2, u).wait()

        @pl.when(n >= SLOTS)
        def _():
            for j in range(len(parts)):
                outgoing(n - SLOTS, j, finish)

        @pl.when(n >= 2 - u)
        def _():
            h_copy(0, u).wait()

        if u == 0:

            @pl.when(t == 0)
            def _():
                h_in = pltpu.make_async_copy(h0.at[k], fb[v].at[5], i_sem.at[0])
                c_in = pltpu.make_async_copy(c0.at[k], cell, i_sem.at[1])
                @pl.when(n > 0)
                def _():
                    h_copy(n - 1, v).wait()
                    f_copy(n - 1, v).wait()

                h_in.start()
                c_in.start()

                spread_bias(k)
                h_in.wait()
                c_in.wait()
                hb[v][0:n_hid, :] = fb[v][5, :, :].astype(BF16)
                pltpu.make_async_copy(hb[v].at[valid], h_seq.at[k, 0], h_sem.at[v]).start()

            every = n_steps // (2 * n_cut)

            @pl.when((n < n_steps) & (lax.rem(n, every) == 0))
            def _():
                transpose_unit(1, n // every)

        arrive(n)
        store_x(n).start()

        @pl.when(n + 1 < n_total)
        def _():
            fetch(n + 1)

        for j, (first, size) in enumerate(blocks):
            gate_rows = pl.ds(4 * first, 4 * size)
            z = zb[j % len(zb)]
            z[0:4 * size, :] = jnp.dot(wt[0, k, gate_rows, :], ring[slot], preferred_element_type=F32) + jnp.dot(wt[1, k, gate_rows, :], hb[v][...], preferred_element_type=F32)
            for r, count in _chunks(first, size):
                rows = pl.ds(r, count)
                pre = []
                for g in range(4):
                    at = g * size + r - first
                    pre.append(z[at:at + count, :] + jnp.concatenate([bias[4 * first + at:4 * first + at + count, :]] * 2, axis=1))
                gate_i = 0.5 * jnp.tanh(pre[0]) + 0.5
                gate_f = 0.5 * jnp.tanh(pre[1]) + 0.5
                gate_g = jnp.tanh(pre[2])
                gate_o = 0.5 * jnp.tanh(pre[3]) + 0.5
                c_old = cell[rows, :]
                c_new = gate_f * c_old + gate_i * gate_g
                tanh_c = jnp.tanh(c_new)
                h_wide = gate_o * tanh_c
                h_new = h_wide.astype(BF16)
                cell[rows, :] = c_new
                hb[u][rows, :] = h_new
                ob[slot, rows, :] = (ring[slot, rows, :].astype(F32) + h_new.astype(F32)).astype(BF16)
                fb[u][0, rows, :] = gate_i * gate_g * (1.0 - gate_i)
                fb[u][1, rows, :] = gate_f * c_old * (1.0 - gate_f)
                fb[u][2, rows, :] = gate_i * (1.0 - gate_g * gate_g)
                fb[u][3, rows, :] = h_wide * (1.0 - gate_o)
                fb[u][4, rows, :] = gate_o * (1.0 - tanh_c * tanh_c)
                fb[u][5, rows, :] = gate_f

        @pl.when(jnp.logical_not(is_last) & (n >= SLOTS))
        def _():
            pl.semaphore_wait(free_sem, 1)

        for j in range(len(parts)):
            outgoing(n, j, start)
        f_copy(n, u).start()
        h_copy(n, u).start()

        @pl.when(n >= 1)
        def _():
            store_x(n - 1).wait()

        @pl.when(jnp.logical_not(is_first) & (n >= 1) & (n <= n_total - SLOTS))
        def _():
            pl.semaphore_signal(free_sem, inc=1, device_id={'pp': prv}, device_id_type=MESH)

    def pair(i, carry):
        step(2 * i, 0)
        step(2 * i + 1, 1)
        return carry

    lax.fori_loop(0, n_steps, pair, 0)
    store_x(n_total - 1).wait()
    for n in range(n_total - SLOTS, n_total):
        for j in range(len(parts)):
            outgoing(n, j, finish)
    for n, u in ((n_total - 2, 0), (n_total - 1, 1)):
        f_copy(n, u).wait()
        h_copy(n, u).wait()


def _bwd_kernel(n_stages, n_steps, n_hid, scale, saved, h_seq, top, target, wx_hbm, wh_hbm, wrap, dz_seq, dwh, db, dh_out, dc_out, loss, wx, wh, acc, zb0, zb1, fb0, fb1, ring, tb0, tb1, ob0, ob1, hb0, hb1, dh, dc, gin, bacc, lacc, lbuf, w_sem, s_sem, a_sem, t_sem, h_sem, z_sem, o_sem, f_sem, recv_sem, wrap_sem, l_sem, free_sem):
    n_total = 2 * n_steps
    n_gate = 4 * n_hid
    blocks = _blocks(n_hid)
    valid = pl.ds(0, n_hid)
    n_tiles = [(n, min(4 * BLK, n_gate - n)) for n in range(0, n_gate, 4 * BLK)]
    zb, fb, tb, ob, hb = (zb0, zb1), (fb0, fb1), (tb0, tb1), (ob0, ob1), (hb0, hb1)

    def weight_copies(k):
        return [pltpu.make_async_copy(wh_hbm.at[k], wh, w_sem.at[0]), pltpu.make_async_copy(wx_hbm.at[k], wx, w_sem.at[1])]

    def place(n):
        return 1 - n // n_steps, n_steps - 1 - lax.rem(n, n_steps)

    def fetch_saved(n, u):
        k, t = place(n)
        pltpu.make_async_copy(saved.at[k, t], fb[u], s_sem.at[u]).start()

    def wait_saved(u):
        pltpu.make_async_copy(saved.at[0, 0], fb[u], s_sem.at[u]).wait()

    def fetch_h(n, u):
        k, t = place(n)
        pltpu.make_async_copy(h_seq.at[k, t], hb[u].at[valid], h_sem.at[u]).start()

    def wait_h(u):
        pltpu.make_async_copy(h_seq.at[0, 0], hb[u].at[valid], h_sem.at[u]).wait()

    for copy in weight_copies(1):
        copy.start()
    fetch_saved(0, 0)
    acc[...] = jnp.zeros_like(acc)
    for buf in (dh, dc, tb0, tb1, zb1, hb0, hb1, lacc, bacc):
        buf[...] = jnp.zeros_like(buf)
    stage, nxt, prv = _enter(n_stages)
    is_first = stage == 0
    is_last = stage == n_stages - 1

    def fetch_grad(n, u):
        k, t = place(n)
        slot = lax.rem(n, SLOTS)

        @pl.when(is_last & (k == 1))
        def _():
            pltpu.make_async_copy(top.at[t], ring.at[slot], a_sem.at[slot]).start()
            pltpu.make_async_copy(target.at[t], tb[u], t_sem.at[u]).start()

        @pl.when(is_last & (k == 0))
        def _():
            pltpu.make_async_remote_copy(src_ref=ob0, dst_ref=wrap.at[t], send_sem=o_sem.at[0, 0], recv_sem=wrap_sem.at[t], device_id={'pp': prv}, device_id_type=MESH).wait_recv()
            pltpu.make_async_copy(wrap.at[t], ring.at[slot], a_sem.at[slot]).start()

    def wait_grad(n, u):
        slot = lax.rem(n, SLOTS)

        @pl.when(is_last)
        def _():
            pltpu.make_async_copy(top.at[0], ring.at[slot], a_sem.at[slot]).wait()

        @pl.when(is_last & (n < n_steps))
        def _():
            pltpu.make_async_copy(target.at[0], tb[u], t_sem.at[u]).wait()

        @pl.when(jnp.logical_not(is_last))
        def _():
            pltpu.make_async_remote_copy(src_ref=ob0, dst_ref=ring.at[slot], send_sem=o_sem.at[0, 0], recv_sem=recv_sem.at[slot], device_id={'pp': prv}, device_id_type=MESH).wait_recv()

    def outgoing(n, u, j, act):
        k, t = place(n)
        slot = lax.rem(n, SLOTS)
        rows = pl.ds(*blocks[j])

        @pl.when(jnp.logical_not(is_first))
        def _():
            act(pltpu.make_async_remote_copy(src_ref=ob[u].at[rows], dst_ref=ring.at[slot, rows], send_sem=o_sem.at[u, j], recv_sem=recv_sem.at[slot], device_id={'pp': prv}, device_id_type=MESH))

        @pl.when(is_first & (k == 1))
        def _():
            act(pltpu.make_async_remote_copy(src_ref=ob[u].at[rows], dst_ref=wrap.at[t, rows], send_sem=o_sem.at[u, j], recv_sem=wrap_sem.at[t], device_id={'pp': prv}, device_id_type=MESH))

    def dz_copy(n, u):
        k, t = place(n)
        return pltpu.make_async_copy(zb[u], dz_seq.at[k, t], z_sem.at[u])

    def weight_grad(v, i):
        n, m = n_tiles[i]
        acc[:, n:n + m] += lax.dot_general(hb[v][...], zb[v][n:n + m, :], ALONG_LANES, preferred_element_type=F32)

    def acc_copy(k):
        return pltpu.make_async_copy(acc.at[valid], dwh.at[k], f_sem.at[0])

    def state_copies(k):
        return [pltpu.make_async_copy(dh, dh_out.at[k], f_sem.at[1]), pltpu.make_async_copy(dc, dc_out.at[k], f_sem.at[2])]

    fetch_h(0, 0)

    def relay():
        return pltpu.make_async_remote_copy(src_ref=lbuf, dst_ref=lbuf, send_sem=l_sem.at[0], recv_sem=l_sem.at[1], device_id={'pp': prv}, device_id_type=MESH)

    fetch_grad(0, 0)
    for copy in weight_copies(1):
        copy.wait()

    def step(n, u):
        k, t = place(n)
        slot = lax.rem(n, SLOTS)
        v = 1 - u
        if u == 0:

            @pl.when(n == n_steps)
            def _():
                for copy in weight_copies(0) + state_copies(1):
                    copy.start()
                for copy in state_copies(1):
                    copy.wait()
                for buf in (dh, dc, tb0, tb1):
                    buf[...] = jnp.zeros_like(buf)
                for copy in weight_copies(0):
                    copy.wait()

        else:

            @pl.when(n == n_steps + 1)
            def _():
                acc_copy(1).wait()
                acc[...] = jnp.zeros_like(acc)

        @pl.when(n >= 2)
        def _():
            dz_copy(n - 2, u).wait()
            for j in range(len(blocks)):
                outgoing(n - 2, u, j, lambda copy: copy.wait_send())

        if u == 0:

            @pl.when(n > 0)
            def _():
                wait_h(v)
        else:
            wait_h(v)
        wait_saved(u)
        wait_grad(n, u)

        @pl.when(n + 1 < n_total)
        def _():
            fetch_saved(n + 1, v)
            fetch_grad(n + 1, v)

        mult = jnp.where(is_last & (k == 1), scale, 1.0).astype(F32)
        for i, (first, size) in enumerate(blocks):
            weight_grad(v, i)
            square = jnp.zeros((8, BLK), F32)
            for r, count in _chunks(first, size):
                rows = pl.ds(r, count)
                diff = ring[slot, rows, :].astype(F32) - tb[u][rows, :].astype(F32)
                for e in range(0, count, 8):
                    square = square + diff[e:e + 8] * diff[e:e + 8]
                into = diff * mult
                gin[rows, :] = into
                dh_all = into + dh[rows, :]
                dc_all = dc[rows, :] + dh_all * fb[u][4, rows, :]
                dc[rows, :] = dc_all * fb[u][5, rows, :]
                for g in range(4):
                    dz = (dh_all if g == 3 else dc_all) * fb[u][g, rows, :]
                    at = pl.ds(g * n_hid + r, count)
                    bacc[k, at, :] += dz[:, :LANES] + dz[:, LANES:]
                    zb[u][at, :] = dz.astype(BF16)
            lacc[...] += square
            if i + 1 < len(blocks):
                hb[v][n_hid:, :] = zb[u][first + size - 8:first + size, :]
        for first, size in blocks:
            dh[pl.ds(first, size), :] = jnp.dot(wh[pl.ds(first, size), :], zb[u][...], preferred_element_type=F32)
        for first, size in blocks:
            rows = pl.ds(first, size)
            ob[u][rows, :] = (gin[rows, :] + jnp.dot(wx[rows, :], zb[u][...], preferred_element_type=F32)).astype(BF16)

        @pl.when(jnp.logical_not(is_first) & (n >= SLOTS))
        def _():
            pl.semaphore_wait(free_sem, 1)

        for j in range(len(blocks)):
            outgoing(n, u, j, lambda copy: copy.start())
        dz_copy(n, u).start()

        @pl.when(jnp.logical_not(is_last) & (n < n_total - SLOTS))
        def _():
            pl.semaphore_signal(free_sem, inc=1, device_id={'pp': nxt}, device_id_type=MESH)

        @pl.when(n + 1 < n_total)
        def _():
            fetch_h(n + 1, v)

        if u == 0:

            @pl.when(n == n_steps)
            def _():
                acc_copy(1).start()

        else:

            @pl.when(is_last & (n == n_steps - 1))
            def _():
                lbuf[...] = lacc[...]
                relay().start()

            @pl.when(jnp.logical_not(is_last) & (n == n_steps + 1))
            def _():
                relay().wait_recv()

                @pl.when(jnp.logical_not(is_first))
                def _():
                    relay().start()

    def pair(i, carry):
        step(2 * i, 0)
        step(2 * i + 1, 1)
        return carry

    lax.fori_loop(0, n_steps, pair, 0)
    wait_h(1)
    last = []
    for i, (n, m) in enumerate(n_tiles):
        weight_grad(1, i)
        last.append(pltpu.make_async_copy(acc.at[valid, pl.ds(n, m)], dwh.at[0, :, pl.ds(n, m)], w_sem.at[i]))
        last[-1].start()
    flush = [pltpu.make_async_copy(bacc, db, f_sem.at[3]), pltpu.make_async_copy(lbuf, loss, f_sem.at[4])] + state_copies(0)
    for copy in flush:
        copy.start()
    for n, u in ((n_total - 2, 0), (n_total - 1, 1)):
        dz_copy(n, u).wait()
        for j in range(len(blocks)):
            outgoing(n, u, j, lambda copy: copy.wait_send())

    @pl.when(jnp.logical_not(is_first))
    def _():
        relay().wait_send()

    for copy in last + flush:
        copy.wait()


def _dense_kernel(n_chunk, half, r_ref, z_ref, dwh_in, db_in, dh_in, dc_in, loss_in, dwx_ref, dwh_ref, db_ref, dh_ref, dc_ref, loss_ref):
    @pl.when(pl.program_id(2) == 0)
    def _():
        dwx_ref[...] = jnp.zeros_like(dwx_ref)
        loss_ref[...] = half * jnp.sum(jnp.sum(loss_in[...], axis=0, keepdims=True), axis=1, keepdims=True)

    n_gate = dwx_ref.shape[-1]
    for n in range(0, n_gate, 4 * BLK):
        m = min(4 * BLK, n_gate - n)
        dwx_ref[0, :, n:n + m] += sum(lax.dot_general(r_ref[0, t], z_ref[0, t, n:n + m, :], ALONG_LANES, preferred_element_type=F32) for t in range(n_chunk))
    dwh_ref[...] = dwh_in[...]
    dh_ref[...] = dh_in[...]
    dc_ref[...] = dc_in[...]
    for n in range(0, db_in.shape[1], LANES):
        db_ref[0, :, n:n + LANES] = jnp.sum(db_in[0, n:n + LANES, :].T, axis=0, keepdims=True)


def solution(mesh):
    n_stages = mesh.shape['pp']

    def local_fn(inputs, targets, w_in, w_hid, bias, h_init, c_init):
        n_batch, n_steps, n_hid = inputs.shape
        n_gate = 4 * n_hid
        n_pad = -(-n_hid // BLK) * BLK
        n_blk = len(_blocks(n_hid))
        seq0 = jnp.transpose(inputs, (1, 2, 0))
        target = jnp.transpose(targets, (1, 2, 0))
        h0 = jnp.transpose(h_init[:, 0], (0, 2, 1))
        c0 = jnp.transpose(c_init[:, 0], (0, 2, 1))
        wx, wh = w_in[:, 0], w_hid[:, 0]

        def shape(*dims, dtype=BF16):
            return jax.ShapeDtypeStruct(dims, dtype)

        any_spec = pl.BlockSpec(memory_space=pl.ANY)
        vmem_spec = pl.BlockSpec(memory_space=pltpu.VMEM)
        row = (n_hid, n_batch)
        wide = (n_pad, n_batch)
        tall = (n_gate, n_batch)
        dma = pltpu.SemaphoreType.DMA
        step_flops = 2 * n_batch * n_hid * n_gate
        _, r_seq, h_seq, saved, top = pl.pallas_call(
            functools.partial(_fwd_kernel, n_stages, n_steps, n_hid),
            out_shape=(shape(n_steps, *row), shape(2, n_steps, *row), shape(2, n_steps + 1, *row), shape(2, n_steps, 6, *row, dtype=F32), shape(n_steps, *row)),
            in_specs=[any_spec, any_spec, any_spec, vmem_spec, any_spec, any_spec],
            out_specs=[any_spec] * 5,
            scratch_shapes=[pltpu.VMEM((2, 2, n_gate, n_pad), BF16), pltpu.VMEM((2, BLK, n_gate), BF16), pltpu.VMEM((BLK, BLK), BF16), pltpu.VMEM((n_gate, LANES), F32), pltpu.VMEM((SLOTS, *wide), BF16)] + [pltpu.VMEM(wide, BF16)] * 2 + [pltpu.VMEM(row, F32)] + [pltpu.VMEM((4 * FINE, n_batch), F32)] * 2 + [pltpu.VMEM((6, *row), F32)] * 2 + [pltpu.VMEM((SLOTS, *row), BF16)] + [dma((2,)), dma((SLOTS,)), dma((SLOTS,)), dma((2,)), dma((2,)), dma((SLOTS, n_blk)), dma((2,)), dma((SLOTS,)), dma((n_steps,)), pltpu.SemaphoreType.REGULAR],
            compiler_params=pltpu.CompilerParams(collective_id=0, has_side_effects=True, vmem_limit_bytes=VMEM_LIMIT),
            cost_estimate=pl.CostEstimate(flops=4 * n_steps * step_flops, bytes_accessed=0, transcendentals=0),
            name='lstm_forward',
        )(seq0, wx, wh, bias, h0, c0)

        scale = 1.0 / (n_batch * n_steps)
        _, dz_seq, dwh_p, db_p, dh_p, dc_p, loss_p = pl.pallas_call(
            functools.partial(_bwd_kernel, n_stages, n_steps, n_hid, scale),
            out_shape=(shape(n_steps, *row), shape(2, n_steps, *tall), shape(2, n_hid, n_gate, dtype=F32), shape(2, n_gate, LANES, dtype=F32), shape(2, *row, dtype=F32), shape(2, *row, dtype=F32), shape(8, n_batch, dtype=F32)),
            in_specs=[any_spec] * 6,
            out_specs=[any_spec] * 7,
            scratch_shapes=[pltpu.VMEM((n_hid, n_gate), BF16)] * 2 + [pltpu.VMEM((n_hid + 8, n_gate), F32)] + [pltpu.VMEM(tall, BF16)] * 2 + [pltpu.VMEM((6, *row), F32)] * 2 + [pltpu.VMEM((SLOTS, *row), BF16)] + [pltpu.VMEM(row, BF16)] * 4 + [pltpu.VMEM((n_hid + 8, n_batch), BF16)] * 2 + [pltpu.VMEM(row, F32)] * 3 + [pltpu.VMEM((2, n_gate, LANES), F32)] + [pltpu.VMEM((8, n_batch), F32)] * 2 + [dma((n_blk,)), dma((2,)), dma((SLOTS,)), dma((2,)), dma((2,)), dma((2,)), dma((2, n_blk)), dma((5,)), dma((SLOTS,)), dma((n_steps,)), dma((2,)), pltpu.SemaphoreType.REGULAR],
            compiler_params=pltpu.CompilerParams(collective_id=1, has_side_effects=True, vmem_limit_bytes=VMEM_LIMIT),
            cost_estimate=pl.CostEstimate(flops=6 * n_steps * step_flops, bytes_accessed=0, transcendentals=0),
            name='lstm_backward',
        )(saved, h_seq, top, target, wx, wh)

        n_chunk = 4
        n_part = 2 * n_steps // n_chunk
        p_rows = n_pad // n_part
        half_gate = n_blk * BLK * 2
        part = lambda k, h, c: (k, h * (n_steps // n_chunk) + c, 0)
        dwx, dwh, db, dh, dc, loss = pl.pallas_call(
            functools.partial(_dense_kernel, n_chunk, 0.5 * scale),
            grid=(2, 2, n_steps // n_chunk),
            out_shape=(shape(2, n_hid, n_gate, dtype=F32), shape(2, n_hid, n_gate, dtype=F32), shape(2, 1, n_gate, dtype=F32), shape(2, *row, dtype=F32), shape(2, *row, dtype=F32), shape(1, 1, dtype=F32)),
            in_specs=[pl.BlockSpec((1, n_chunk, *row), lambda k, h, c: (k, c, 0, 0)), pl.BlockSpec((1, n_chunk, half_gate, n_batch), lambda k, h, c: (k, c, h, 0)), pl.BlockSpec((1, p_rows, n_gate), part), pl.BlockSpec((1, 4 * p_rows, LANES), part), pl.BlockSpec((1, p_rows, n_batch), part), pl.BlockSpec((1, p_rows, n_batch), part), pl.BlockSpec((8, n_batch), lambda k, h, c: (0, 0))],
            out_specs=[pl.BlockSpec((1, n_hid, half_gate), lambda k, h, c: (k, 0, h)), pl.BlockSpec((1, p_rows, n_gate), part), pl.BlockSpec((1, 1, 4 * p_rows), lambda k, h, c: (k, 0, h * (n_steps // n_chunk) + c)), pl.BlockSpec((1, p_rows, n_batch), part), pl.BlockSpec((1, p_rows, n_batch), part), pl.BlockSpec((1, 1), lambda k, h, c: (0, 0))],
            compiler_params=pltpu.CompilerParams(dimension_semantics=('arbitrary', 'arbitrary', 'arbitrary'), vmem_limit_bytes=VMEM_LIMIT),
            cost_estimate=pl.CostEstimate(flops=2 * n_steps * step_flops, bytes_accessed=0, transcendentals=0),
            name='input_weight_grad',
        )(r_seq, dz_seq, dwh_p, db_p, dh_p, dc_p, loss_p)

        back = lambda g: jnp.transpose(g, (0, 2, 1))[:, None]
        return loss[0], dwx[:, None], dwh[:, None], db, back(dh), back(dc)

    spec_seq = P('dp', None, None)
    spec_weight = P('dp', 'pp', None, None)
    spec_bias = P('dp', 'pp', None)
    return jax.shard_map(local_fn, mesh=mesh, in_specs=(spec_seq, spec_seq, spec_weight, spec_weight, spec_bias, spec_weight, spec_weight), out_specs=(P('dp'), spec_weight, spec_weight, spec_bias, spec_weight, spec_weight), check_vma=False)
```
